32 devices in a mesh: dp: 1 (over z), dpa: 32 (over y, x, core).
Axes of the slice: x: 4, y: 4, z: 1, core: 2. Of those that a mesh axis runs over, the one named last changes fastest.
The devices are a block of a 4x4x8 slice.
Arguments:
- x: bfloat16 [32, 1, 512, 2048], P(('dp', 'dpa'))
- chunk_len: int32 [32, 1], P(('dp', 'dpa'))
- ctx_len: int32 [32, 1], P(('dp', 'dpa'))
- lat_cache: bfloat16 [32, 1, 1024, 512], P(('dp', 'dpa'))
- rope_cache: bfloat16 [32, 1, 1024, 64], P(('dp', 'dpa'))
- topk_idx: int32 [32, 1, 512, 6], P(('dp', 'dpa'))
- g_attn: bfloat16 [2048], replicated
- w_q: bfloat16 [2048, 16, 192], replicated
- w_dkv: bfloat16 [2048, 512], replicated
- g_kv: bfloat16 [512], replicated
- w_kr: bfloat16 [2048, 64], replicated
- w_uk: bfloat16 [512, 16, 128], replicated
- w_uv: bfloat16 [512, 16, 128], replicated
- w_o: bfloat16 [16, 128, 2048], replicated
- g_ffn: bfloat16 [2048], replicated
- w_router: bfloat16 [2048, 64], replicated
- w_sh_gate: bfloat16 [2048, 2816], replicated
- w_sh_up: bfloat16 [2048, 2816], replicated
- w_sh_down: bfloat16 [2816, 2048], replicated
- w_exp_gate: bfloat16 [64, 2048, 1408], P('dpa')
- w_exp_up: bfloat16 [64, 2048, 1408], P('dpa')
- w_exp_down: bfloat16 [64, 1408, 2048], P('dpa')
Outputs:
- output 1: bfloat16 [32, 1, 512, 2048], P(('dp', 'dpa'))
- output 2: bfloat16 [32, 1, 1024, 512], P(('dp', 'dpa'))
- output 3: bfloat16 [32, 1, 1024, 64], P(('dp', 'dpa'))
All inputs are finite; a program needn't handle non-finite values.
Results may differ from the reference program's by a relative error of at most 0.0196077.
Values are sent between devices in bfloat16 or wider.
A program may use at most 768 MiB of HBM per device.

```python
import jax
import jax.numpy as jnp
from jax import lax

GROUP = 32
REQS = 1
CHUNK = 512
CTX = 1024
HID = 2048
HEADS = 16
NOPE = 128
ROPE = 64
VDIM = 128
RANK = 512
EXPERTS = 64
EXP_FF = 1408
SHARED_FF = 2816
TOP = 6
BLOCK_ROWS = 128

TOKENS = REQS * CHUNK
LOCAL = EXPERTS // GROUP
QDIM = NOPE + ROPE
EPS = 1e-6
THETA = 10000.0


def draw_normal(rand_key, shape, scale):
    return (jax.random.normal(rand_key, shape, jnp.float32) * scale).astype(jnp.bfloat16)


def draw_gain(rand_key, width):
    return jax.random.uniform(rand_key, (width,), jnp.float32, 0.5, 1.5).astype(jnp.bfloat16)


def draw_lengths(rand_key):
    chunk_key, ctx_key = jax.random.split(rand_key)
    chunk_len = jax.random.randint(chunk_key, (GROUP, REQS), CHUNK // 4, CHUNK + 1).astype(jnp.int32)
    ctx_len = jax.random.randint(ctx_key, (GROUP, REQS), CTX // 8, CTX - CHUNK + 1).astype(jnp.int32)
    return chunk_len.at[0, 0].set(CHUNK), ctx_len.at[GROUP - 1, REQS - 1].set(CTX - CHUNK)


def draw_routes(rand_key):
    start_key, local_key = jax.random.split(rand_key)
    shuffled = jax.vmap(lambda sub_key: jax.random.permutation(sub_key, TOKENS))(jax.random.split(start_key, GROUP))
    first_dev = shuffled % GROUP
    first_loc = jax.random.randint(local_key, (GROUP, TOKENS), 0, LOCAL)
    slot_ids = jnp.arange(TOP)
    target = (first_dev[:, :, None] + slot_ids) % GROUP
    local_id = (first_loc[:, :, None] + slot_ids // GROUP) % LOCAL
    return (target * LOCAL + local_id).reshape(GROUP, REQS, CHUNK, TOP).astype(jnp.int32)


def setup_inputs(seed: int = 0, part: int = 0) -> dict:
    base_key = jax.random.key(seed)
    part_keys = jax.random.split(jax.random.fold_in(base_key, part), 6)
    shared_keys = jax.random.split(base_key, 16)
    chunk_len, ctx_len = draw_lengths(part_keys[0])
    return {
        'x': draw_normal(part_keys[1], (GROUP, REQS, CHUNK, HID), 1.0),
        'chunk_len': chunk_len,
        'ctx_len': ctx_len,
        'lat_cache': draw_normal(part_keys[2], (GROUP, REQS, CTX, RANK), 1.0),
        'rope_cache': draw_normal(part_keys[3], (GROUP, REQS, CTX, ROPE), 1.0),
        'topk_idx': draw_routes(part_keys[4]),
        'g_attn': draw_gain(shared_keys[0], HID),
        'w_q': draw_normal(shared_keys[1], (HID, HEADS, QDIM), HID ** -0.5),
        'w_dkv': draw_normal(shared_keys[2], (HID, RANK), HID ** -0.5),
        'g_kv': draw_gain(shared_keys[3], RANK),
        'w_kr': draw_normal(shared_keys[4], (HID, ROPE), HID ** -0.5),
        'w_uk': draw_normal(shared_keys[5], (RANK, HEADS, NOPE), 2.5 * NOPE ** -0.5),
        'w_uv': draw_normal(shared_keys[6], (RANK, HEADS, VDIM), RANK ** -0.5),
        'w_o': draw_normal(shared_keys[7], (HEADS, VDIM, HID), 4.0 * (HEADS * VDIM) ** -0.5),
        'g_ffn': draw_gain(shared_keys[8], HID),
        'w_router': draw_normal(shared_keys[9], (HID, EXPERTS), HID ** -0.5),
        'w_sh_gate': draw_normal(shared_keys[10], (HID, SHARED_FF), HID ** -0.5),
        'w_sh_up': draw_normal(shared_keys[11], (HID, SHARED_FF), HID ** -0.5),
        'w_sh_down': draw_normal(shared_keys[12], (SHARED_FF, HID), SHARED_FF ** -0.5),
        'w_exp_gate': draw_normal(shared_keys[13], (EXPERTS, HID, EXP_FF), HID ** -0.5),
        'w_exp_up': draw_normal(shared_keys[14], (EXPERTS, HID, EXP_FF), HID ** -0.5),
        'w_exp_down': draw_normal(shared_keys[15], (EXPERTS, EXP_FF, HID), 0.8 * EXPERTS * EXP_FF ** -0.5),
    }


def rms_norm(vals, gain):
    vals_f32 = vals.astype(jnp.float32)
    inv_rms = lax.rsqrt(jnp.mean(vals_f32 * vals_f32, axis=-1, keepdims=True) + EPS)
    return (vals_f32 * inv_rms * gain.astype(jnp.float32)).astype(jnp.bfloat16)


def rope_tables(positions):
    inv_freq = THETA ** (-2.0 * jnp.arange(ROPE // 2, dtype=jnp.float32) / ROPE)
    angle = positions.astype(jnp.float32)[..., None] * inv_freq
    return jnp.cos(angle), jnp.sin(angle)


def rotate(vals, cos_tab, sin_tab):
    half = ROPE // 2
    first = vals[..., :half]
    second = vals[..., half:]
    return jnp.concatenate([first * cos_tab - second * sin_tab, second * cos_tab + first * sin_tab], axis=-1)


def write_window(cache_row, new_rows, start, keep):
    old_rows = lax.dynamic_slice_in_dim(cache_row, start, CHUNK, axis=0)
    merged = jnp.where(keep[:, None], new_rows, old_rows)
    return lax.dynamic_update_slice_in_dim(cache_row, merged, start, axis=0)


def reference(x, chunk_len, ctx_len, lat_cache, rope_cache, topk_idx, g_attn, w_q, w_dkv, g_kv, w_kr, w_uk, w_uv, w_o, g_ffn, w_router, w_sh_gate, w_sh_up, w_sh_down, w_exp_gate, w_exp_up, w_exp_down):
    def one_request(args):
        x_req, req_chunk, req_ctx, lat_old, rope_old = args
        normed = rms_norm(x_req, g_attn)
        q_full = jnp.dot(normed, w_q.reshape(HID, HEADS * QDIM), preferred_element_type=jnp.float32).astype(jnp.bfloat16).reshape(CHUNK, HEADS, QDIM)
        positions = req_ctx + jnp.arange(CHUNK)
        cos_tab, sin_tab = rope_tables(positions)
        q_rope = rotate(q_full[:, :, NOPE:].astype(jnp.float32), cos_tab[:, None, :], sin_tab[:, None, :]).astype(jnp.bfloat16)
        q_lat = jnp.einsum('chn,khn->chk', q_full[:, :, :NOPE].astype(jnp.float32), w_uk.astype(jnp.float32)).astype(jnp.bfloat16)
        lat_new = rms_norm(jnp.dot(normed, w_dkv, preferred_element_type=jnp.float32), g_kv)
        rope_new = rotate(jnp.dot(normed, w_kr, preferred_element_type=jnp.float32), cos_tab, sin_tab).astype(jnp.bfloat16)
        keep = jnp.arange(CHUNK) < req_chunk
        lat_upd = write_window(lat_old, lat_new, req_ctx, keep)
        rope_upd = write_window(rope_old, rope_new, req_ctx, keep)
        lat_f32 = lat_upd.astype(jnp.float32)
        scores = (jnp.einsum('chk,lk->chl', q_lat.astype(jnp.float32), lat_f32) + jnp.einsum('chp,lp->chl', q_rope.astype(jnp.float32), rope_upd.astype(jnp.float32))) * QDIM ** -0.5
        visible = jnp.arange(CTX)[None, None, :] <= positions[:, None, None]
        scores = jnp.where(visible, scores, -1e30)
        attn_prob = jax.nn.softmax(scores, axis=-1).astype(jnp.bfloat16)
        out_lat = jnp.einsum('chl,lk->chk', attn_prob.astype(jnp.float32), lat_f32).astype(jnp.bfloat16)
        out_head = jnp.einsum('chk,khv->chv', out_lat.astype(jnp.float32), w_uv.astype(jnp.float32)).astype(jnp.bfloat16)
        attn_out = jnp.dot(out_head.reshape(CHUNK, HEADS * VDIM), w_o.reshape(HEADS * VDIM, HID), preferred_element_type=jnp.float32).astype(jnp.bfloat16)
        hidden = (x_req.astype(jnp.float32) + attn_out.astype(jnp.float32)).astype(jnp.bfloat16)
        return hidden, lat_upd, rope_upd

    reqs_all = GROUP * REQS
    hidden, lat_upd, rope_upd = lax.map(one_request, (x.reshape(reqs_all, CHUNK, HID), chunk_len.reshape(reqs_all), ctx_len.reshape(reqs_all), lat_cache.reshape(reqs_all, CTX, RANK), rope_cache.reshape(reqs_all, CTX, ROPE)))
    rows = GROUP * TOKENS
    pairs = rows * TOP
    flat_h = hidden.reshape(rows, HID)
    normed = rms_norm(flat_h, g_ffn)
    valid = (jnp.arange(CHUNK)[None, :] < chunk_len.reshape(reqs_all, 1)).reshape(rows)
    route_prob = jax.nn.softmax(jnp.dot(normed, w_router, preferred_element_type=jnp.float32), axis=-1)
    choice = topk_idx.reshape(rows, TOP)
    gates = jnp.take_along_axis(route_prob, choice, axis=1)
    shared_act = (jax.nn.silu(jnp.dot(normed, w_sh_gate, preferred_element_type=jnp.float32)) * jnp.dot(normed, w_sh_up, preferred_element_type=jnp.float32)).astype(jnp.bfloat16)
    shared_out = jnp.dot(shared_act, w_sh_down, preferred_element_type=jnp.float32)
    pair_ok = jnp.repeat(valid, TOP)
    pair_key = jnp.where(pair_ok, choice.reshape(pairs), EXPERTS)
    counts = jnp.bincount(pair_key, length=EXPERTS + 1)
    padded = (counts[:EXPERTS] + BLOCK_ROWS - 1) // BLOCK_ROWS * BLOCK_ROWS
    pad_start = jnp.cumsum(padded) - padded
    raw_start = jnp.cumsum(counts) - counts
    order = jnp.argsort(pair_key, stable=True)
    sorted_key = pair_key[order]
    num_blocks = pairs // BLOCK_ROWS + EXPERTS + 1
    slots = num_blocks * BLOCK_ROWS
    start_ext = jnp.concatenate([pad_start, jnp.full((1,), slots, pad_start.dtype)])
    slot_of_sorted = start_ext[sorted_key] + jnp.arange(pairs) - raw_start[sorted_key]
    slot_pair = jnp.full((slots,), pairs, order.dtype).at[slot_of_sorted].set(order, mode='drop')
    slot_token = slot_pair // TOP
    gate_ext = jnp.concatenate([gates.reshape(pairs), jnp.zeros((1,), jnp.float32)])
    slot_gate = gate_ext[slot_pair]
    block_start = jnp.arange(num_blocks) * BLOCK_ROWS
    block_exp = jnp.clip(jnp.sum(pad_start[None, :] <= block_start[:, None], axis=1) - 1, 0, EXPERTS - 1)
    normed_ext = jnp.concatenate([normed, jnp.zeros((1, HID), jnp.bfloat16)])

    def expert_block(routed, args):
        tok_ids, tok_gate, exp_id = args
        block_in = normed_ext[tok_ids].astype(jnp.float32)
        gate_w = lax.dynamic_index_in_dim(w_exp_gate, exp_id, 0, keepdims=False).astype(jnp.float32)
        up_w = lax.dynamic_index_in_dim(w_exp_up, exp_id, 0, keepdims=False).astype(jnp.float32)
        down_w = lax.dynamic_index_in_dim(w_exp_down, exp_id, 0, keepdims=False).astype(jnp.float32)
        act = (jax.nn.silu(jnp.dot(block_in, gate_w)) * jnp.dot(block_in, up_w)).astype(jnp.bfloat16)
        block_out = jnp.dot(act.astype(jnp.float32), down_w).astype(jnp.bfloat16)
        routed = routed.at[tok_ids].add(tok_gate[:, None] * block_out.astype(jnp.float32), mode='drop')
        return routed, tok_ids[0]

    routed = lax.scan(expert_block, jnp.zeros((rows, HID), jnp.float32), (slot_token.reshape(num_blocks, BLOCK_ROWS), slot_gate.reshape(num_blocks, BLOCK_ROWS), block_exp))[0]
    total = flat_h.astype(jnp.float32) + shared_out + routed
    result = jnp.where(valid[:, None], total, 0.0).astype(jnp.bfloat16).reshape(GROUP, REQS, CHUNK, HID)
    return result, lat_upd.reshape(GROUP, REQS, CTX, RANK), rope_upd.reshape(GROUP, REQS, CTX, ROPE)
```

```python
import functools

import jax
import jax.numpy as jnp
from jax import lax
from jax.experimental import pallas as pl
from jax.experimental.pallas import tpu as pltpu
from jax.sharding import PartitionSpec as P

EPS = 1e-6
THETA = 10000.0
UNIT = 16
STAGES = 2
TILE = 256
BIG = 60000000


def rms_norm(vals, gain):
    vals_f32 = vals.astype(jnp.float32)
    inv_rms = lax.rsqrt(jnp.mean(vals_f32 * vals_f32, axis=-1, keepdims=True) + EPS)
    return (vals_f32 * inv_rms * gain.astype(jnp.float32)).astype(jnp.bfloat16)


def nn_dot(lhs, rhs):
    return jnp.dot(lhs, rhs, preferred_element_type=jnp.float32)


def params(vmem=BIG):
    return pltpu.CompilerParams(vmem_limit_bytes=vmem)


def attn_kernel(ctx_ref, q_ref, uk_ref, uv_ref, lat_ref, kr_ref, cos_ref, sin_ref, out_ref, lat_t_ref, *, scale, nope):
    @pl.when(pl.program_id(0) == 0)
    def _():
        lat_t_ref[...] = lat_ref[...].T

    chunk = q_ref.shape[2]
    half = cos_ref.shape[0]
    block = min(TILE, chunk)
    for r in range(chunk // block):
        cols = slice(r * block, (r + 1) * block)
        q_lat = nn_dot(uk_ref[...], q_ref[0, :nope, cols]).astype(jnp.bfloat16)
        first = q_ref[0, nope:nope + half, cols].astype(jnp.float32)
        second = q_ref[0, nope + half:, cols].astype(jnp.float32)
        cos_tab, sin_tab = cos_ref[:, cols], sin_ref[:, cols]
        q_rope = jnp.concatenate([first * cos_tab - second * sin_tab, second * cos_tab + first * sin_tab], axis=0).astype(jnp.bfloat16)
        scores = (nn_dot(lat_ref[...], q_lat) + nn_dot(kr_ref[...], q_rope)) * scale
        row_pos = lax.broadcasted_iota(jnp.int32, scores.shape, 1) + (ctx_ref[0] + r * block)
        key_pos = lax.broadcasted_iota(jnp.int32, scores.shape, 0)
        scores = jnp.where(key_pos <= row_pos, scores, -1e30)
        expo = jnp.exp(scores - jnp.max(scores, axis=0, keepdims=True))
        prob = (expo * (1.0 / jnp.sum(expo, axis=0, keepdims=True))).astype(jnp.bfloat16)
        out_lat = nn_dot(lat_t_ref[...], prob).astype(jnp.bfloat16)
        out_ref[0, :, cols] = lax.dot_general(uv_ref[...], out_lat, (((0,), (0,)), ((), ())), preferred_element_type=jnp.float32).astype(jnp.bfloat16)


def attention(ctx, q_t, w_uk, w_uv, lat, kr, cos_t, sin_t, scale, nope):
    heads, qdim, chunk = q_t.shape
    keys, rank = lat.shape
    vdim = w_uv.shape[1] // heads
    rope = kr.shape[1]
    full = lambda arr: pl.BlockSpec(arr.shape, lambda h, c: (0, 0))
    head = lambda rows, cols: pl.BlockSpec((1, rows, cols), lambda h, c: (h, 0, 0))
    spec = pltpu.PrefetchScalarGridSpec(
        num_scalar_prefetch=1, grid=(heads,),
        in_specs=[head(qdim, chunk), pl.BlockSpec((rank, nope), lambda h, c: (0, h)), pl.BlockSpec((rank, vdim), lambda h, c: (0, h)),
                  full(lat), full(kr), full(cos_t), full(sin_t)],
        out_specs=head(vdim, chunk), scratch_shapes=[pltpu.VMEM((rank, keys), jnp.bfloat16)])
    flops = 2 * heads * chunk * (rank * (nope + vdim) + keys * (2 * rank + rope))
    return pl.pallas_call(
        functools.partial(attn_kernel, scale=scale, nope=nope), grid_spec=spec,
        out_shape=jax.ShapeDtypeStruct((heads, vdim, chunk), jnp.bfloat16), compiler_params=params(),
        cost_estimate=pl.CostEstimate(flops=flops, bytes_accessed=16 * 2**20, transcendentals=heads * chunk * keys),
        name='attend')(ctx, q_t, w_uk, w_uv, lat, kr, cos_t, sin_t)


def send_kernel(pos_ref, u_ref, out_ref, *, base, top_k):
    tile = out_ref.shape[0]
    tokens = u_ref.shape[0]
    slots = lax.broadcasted_iota(jnp.int32, (tile, tokens), 0) + (base + pl.program_id(0) * tile)
    hit = slots == pos_ref[0:1, :]
    for i in range(1, top_k):
        hit = hit | (slots == pos_ref[i:i + 1, :])
    pick = jnp.where(hit, 1.0, 0.0).astype(jnp.bfloat16)
    out_ref[...] = nn_dot(pick, u_ref[...]).astype(jnp.bfloat16)


def send_rows(pos_t, normed, slots, base, top_k):
    tokens, width = normed.shape
    tile = min(TILE, slots)
    return pl.pallas_call(
        functools.partial(send_kernel, base=base, top_k=top_k), grid=(slots // tile,),
        in_specs=[pl.BlockSpec(pos_t.shape, lambda k: (0, 0)), pl.BlockSpec((tokens, width), lambda k: (0, 0))],
        out_specs=pl.BlockSpec((tile, width), lambda k: (k, 0)),
        out_shape=jax.ShapeDtypeStruct((slots, width), jnp.bfloat16), compiler_params=params(),
        cost_estimate=pl.CostEstimate(flops=2 * slots * tokens * width, bytes_accessed=slots * width * 2, transcendentals=0),
        name='pack_rows')(pos_t, normed)


def expert_kernel(counts_ref, in_ref, gate_hbm, up_hbm, down_hbm, rows_ref, gate_v, up_v, down_v, x_v, y_v, ids, lows, highs, w_sem, in_sem, out_sem, *, first, part, capacity, sources):
    per_tile = x_v.shape[1] // UNIT
    per_source = part // UNIT
    total_units = sources * per_source
    stride = total_units + per_tile
    local_exp = 2

    def weights(e):
        return [pltpu.make_async_copy(src.at[e], dst.at[e], w_sem.at[e]) for src, dst in ((gate_hbm, gate_v), (up_hbm, up_v), (down_hbm, down_v))]

    for e in range(local_exp):
        for copy in weights(e):
            copy.start()

    def list_units(e):
        def step(source, count):
            filled = counts_ref[source, e]
            for j in range(per_source):
                start = first + j * UNIT
                low = 0 if e == 0 else capacity - filled - start
                high = filled - start if e == 0 else UNIT
                ids[e * stride + count] = source * per_source + j
                lows[e * stride + count] = low
                highs[e * stride + count] = high
                need = filled > start if e == 0 else capacity - filled < start + UNIT
                count = count + need.astype(jnp.int32)
            return count
        return lax.fori_loop(0, sources, step, jnp.int32(0))

    units0, units1 = list_units(0), list_units(1)
    tiles0 = lax.div(units0 + (per_tile - 1), per_tile)
    tiles = tiles0 + lax.div(units1 + (per_tile - 1), per_tile)

    def place(t):
        e = jnp.where(t >= tiles0, 1, 0)
        begin = (t - jnp.where(t >= tiles0, tiles0, 0)) * per_tile
        size = jnp.minimum(per_tile, jnp.where(t >= tiles0, units1, units0) - begin)
        return e, e * stride + begin, size

    def in_copy(t, i):
        where = ids[place(t)[1] + i]
        return pltpu.make_async_copy(rows_ref.at[pl.ds(pl.multiple_of(where * UNIT, UNIT), UNIT), :], x_v.at[t % 2, pl.ds(pl.multiple_of(i * UNIT, UNIT), UNIT), :], in_sem.at[t % 2])

    def out_copy(t, i):
        where = ids[place(t)[1] + i]
        return pltpu.make_async_copy(y_v.at[t % 2, pl.ds(pl.multiple_of(i * UNIT, UNIT), UNIT), :], rows_ref.at[pl.ds(pl.multiple_of(where * UNIT, UNIT), UNIT), :], out_sem.at[t % 2])

    def each(t, copy_of, wait):
        @pl.loop(0, place(t)[2])
        def _(i):
            copy = copy_of(t, i)
            copy.wait() if wait else copy.start()

    for copy in weights(0):
        copy.wait()

    @pl.loop(0, tiles)
    def _(t):
        switch = t == tiles0

        @pl.when(switch)
        def _():
            for copy in weights(1):
                copy.wait()

        @pl.when(switch & (t > 0))
        def _():
            each(t - 1, out_copy, True)

        @pl.when(switch | (t == 0))
        def _():
            each(t, in_copy, False)

        each(t, in_copy, True)

        @pl.when((t + 1 < tiles) & (t + 1 != tiles0))
        def _():
            each(t + 1, in_copy, False)

        e, begin, _ = place(t)
        slot = t % 2
        rows = x_v[slot]
        gate = nn_dot(rows, gate_v[e])
        up = nn_dot(rows, up_v[e])
        act = (jax.nn.silu(gate) * up).astype(jnp.bfloat16)
        res = nn_dot(act, down_v[e])
        for i in range(per_tile):
            span = slice(i * UNIT, (i + 1) * UNIT)
            line = lax.broadcasted_iota(jnp.int32, (UNIT, rows.shape[1]), 0)
            mine = (line >= lows[begin + i]) & (line < highs[begin + i])
            y_v[slot, span, :] = jnp.where(mine, res[span], rows[span].astype(jnp.float32)).astype(jnp.bfloat16)

        @pl.when((t > 0) & jnp.logical_not(switch))
        def _():
            each(t - 1, out_copy, True)

        each(t, out_copy, False)

    @pl.when(tiles == tiles0)
    def _():
        for copy in weights(1):
            copy.wait()

    @pl.when(tiles > 0)
    def _():
        each(tiles - 1, out_copy, True)


def expert_rows(counts, rows, w_gate, w_up, w_down, first, part, capacity):
    slots, width = rows.shape
    sources = counts.shape[0]
    local_exp, _, ff = w_gate.shape
    tile = min(TILE, slots)
    room = local_exp * (slots // UNIT + tile // UNIT)
    anywhere = pl.BlockSpec(memory_space=pl.ANY)
    return pl.pallas_call(
        functools.partial(expert_kernel, first=first, part=part, capacity=capacity, sources=sources),
        in_specs=[pl.BlockSpec(memory_space=pltpu.SMEM)] + [anywhere] * 4, out_specs=anywhere,
        out_shape=jax.ShapeDtypeStruct((slots, width), jnp.bfloat16), input_output_aliases={1: 0},
        scratch_shapes=[pltpu.VMEM(w_gate.shape, jnp.bfloat16), pltpu.VMEM(w_up.shape, jnp.bfloat16), pltpu.VMEM(w_down.shape, jnp.bfloat16),
                        pltpu.VMEM((2, tile, width), jnp.bfloat16), pltpu.VMEM((2, tile, width), jnp.bfloat16),
                        pltpu.SMEM((room,), jnp.int32), pltpu.SMEM((room,), jnp.int32), pltpu.SMEM((room,), jnp.int32),
                        pltpu.SemaphoreType.DMA((local_exp,)), pltpu.SemaphoreType.DMA((2,)), pltpu.SemaphoreType.DMA((2,))],
        compiler_params=params(),
        cost_estimate=pl.CostEstimate(flops=6 * slots * width * ff, bytes_accessed=12 * width * ff, transcendentals=0),
        name='expert_rows')(counts, rows, w_gate, w_up, w_down)


def merge_kernel(pos_ref, gate_ref, keep_ref, start_ref, rows_ref, out_ref, acc_ref, *, base, top_k, last):
    k = pl.program_id(0)

    @pl.when(k == 0)
    def _():
        acc_ref[...] = start_ref[...]

    tile = rows_ref.shape[0]
    tokens = acc_ref.shape[0]
    slots = lax.broadcasted_iota(jnp.int32, (tokens, tile), 1) + (base + k * tile)
    mix = jnp.zeros((tokens, tile), jnp.float32)
    for i in range(top_k):
        mix = jnp.where(slots == pos_ref[:, i:i + 1], gate_ref[:, i:i + 1], mix)
    high = mix.astype(jnp.bfloat16)
    rest = mix - high.astype(jnp.float32)
    mid = rest.astype(jnp.bfloat16)
    low = (rest - mid.astype(jnp.float32)).astype(jnp.bfloat16)
    rows = rows_ref[...]
    acc_ref[...] += nn_dot(high, rows) + (nn_dot(mid, rows) + nn_dot(low, rows))

    @pl.when(k == pl.num_programs(0) - 1)
    def _():
        if last:
            out_ref[...] = jnp.where(keep_ref[:, 0:1] > 0, acc_ref[...], 0.0).astype(out_ref.dtype)
        else:
            out_ref[...] = acc_ref[...]


def merge_rows(pos, gates, keep, start, rows, base, top_k, last):
    slots, width = rows.shape
    tokens = start.shape[0]
    tile = min(TILE, slots)
    full = lambda arr: pl.BlockSpec(arr.shape, lambda k: (0, 0))
    return pl.pallas_call(
        functools.partial(merge_kernel, base=base, top_k=top_k, last=last), grid=(slots // tile,),
        in_specs=[full(pos), full(gates), full(keep), full(start), pl.BlockSpec((tile, width), lambda k: (k, 0))],
        out_specs=pl.BlockSpec((tokens, width), lambda k: (0, 0)),
        out_shape=jax.ShapeDtypeStruct((tokens, width), jnp.bfloat16 if last else jnp.float32),
        scratch_shapes=[pltpu.VMEM((tokens, width), jnp.float32)], compiler_params=params(),
        cost_estimate=pl.CostEstimate(flops=6 * slots * tokens * width, bytes_accessed=slots * width * 2, transcendentals=0),
        name='merge_rows')(pos, gates, keep, start, rows)


def solution(mesh):
    group = mesh.shape['dpa']
    tok_spec = P(('dp', 'dpa'))
    whole = P()
    exp_spec = P('dpa')

    def device_step(x_in, chunk_len, ctx_len, lat_cache, rope_cache, topk_idx, g_attn, w_q, w_dkv, g_kv, w_kr, w_uk, w_uv, w_o, g_ffn, w_router, w_sh_gate, w_sh_up, w_sh_down, w_exp_gate, w_exp_up, w_exp_down):
        tokens, width = x_in.shape[2], x_in.shape[3]
        top_k = topk_idx.shape[-1]
        local_exp = w_exp_gate.shape[0]
        experts = group * local_exp
        capacity = tokens * top_k // group
        part = capacity // STAGES
        slots = group * part
        length = chunk_len[0, 0]
        ctx = ctx_len[0, 0]

        row_ids = jnp.arange(tokens, dtype=jnp.int32)
        valid = row_ids < length
        choice = topk_idx.reshape(tokens, top_k)
        picked = (choice[:, :, None] == jnp.arange(experts, dtype=jnp.int32)) & valid[:, None, None]
        member = jnp.any(picked, axis=1)
        before = (row_ids[:, None] > row_ids[None, :]).astype(jnp.bfloat16)
        rank_in = nn_dot(before, member.astype(jnp.bfloat16)).astype(jnp.int32)
        counts = jnp.sum(member.astype(jnp.int32), axis=0)
        counts_in = lax.all_to_all(counts.reshape(group, local_exp), 'dpa', 0, 0, tiled=True)
        ids = jnp.arange(experts, dtype=jnp.int32)
        place = jnp.where(ids % local_exp == 0, rank_in, capacity - 1 - rank_in)
        pos_all = (place // part) * slots + (ids // local_exp) * part + place % part
        pos = jnp.sum(jnp.where(picked, pos_all[:, None, :], 0), axis=2)
        pos = jnp.where(valid[:, None], pos, -1)
        pad_k = (-top_k) % 8
        pos = jnp.pad(pos, ((0, 0), (0, pad_k)), constant_values=-1)
        pos_t = pos.T

        chunk_x = x_in.reshape(tokens, width)
        normed_x = rms_norm(chunk_x, g_attn)
        rope_dim = w_kr.shape[1]
        heads, qdim = w_q.shape[1], w_q.shape[2]
        nope_dim = qdim - rope_dim
        half = rope_dim // 2
        q_t = jnp.einsum('cd,dhq->hqc', normed_x, w_q, preferred_element_type=jnp.float32).astype(jnp.bfloat16)
        inv_freq = THETA ** (-2.0 * jnp.arange(half, dtype=jnp.float32) / (2 * half))
        angle = (ctx + row_ids).astype(jnp.float32)[:, None] * inv_freq
        cos_tab, sin_tab = jnp.cos(angle), jnp.sin(angle)
        lat_new = rms_norm(nn_dot(normed_x, w_dkv), g_kv)
        kr_raw = nn_dot(normed_x, w_kr)
        kr_new = jnp.concatenate([kr_raw[:, :half] * cos_tab - kr_raw[:, half:] * sin_tab, kr_raw[:, half:] * cos_tab + kr_raw[:, :half] * sin_tab], axis=1).astype(jnp.bfloat16)

        def write_window(cache, new_rows):
            old_rows = lax.dynamic_slice_in_dim(cache, ctx, tokens, axis=0)
            return lax.dynamic_update_slice_in_dim(cache, jnp.where(valid[:, None], new_rows, old_rows), ctx, axis=0)

        lat_upd = write_window(lat_cache[0, 0], lat_new)
        rope_upd = write_window(rope_cache[0, 0], kr_new)
        out_head = attention(ctx_len.reshape(1), q_t, w_uk.reshape(w_uk.shape[0], -1), w_uv.reshape(w_uv.shape[0], -1), lat_upd, rope_upd, cos_tab.T, sin_tab.T, qdim ** -0.5, nope_dim)
        attn_out = jnp.einsum('hvc,hvd->cd', out_head, w_o, preferred_element_type=jnp.float32).astype(jnp.bfloat16)
        hidden = (chunk_x.astype(jnp.float32) + attn_out.astype(jnp.float32)).astype(jnp.bfloat16)
        normed = rms_norm(hidden, g_ffn)

        packed = [send_rows(pos_t, normed, slots, h * slots, top_k).reshape(group, part, width) for h in range(STAGES)]
        shared_act = (jax.nn.silu(nn_dot(normed, w_sh_gate)) * nn_dot(normed, w_sh_up)).astype(jnp.bfloat16)
        packed[1], shared_act = lax.optimization_barrier((packed[1], shared_act))
        landed = [lax.all_to_all(rows, 'dpa', 0, 0, tiled=True) for rows in packed]
        total = hidden.astype(jnp.float32) + nn_dot(shared_act, w_sh_down)
        route_prob = jax.nn.softmax(nn_dot(normed, w_router), axis=-1)
        gates = jnp.sum(jnp.where(picked, route_prob[:, None, :], 0.0), axis=2)
        gates = jnp.pad(gates, ((0, 0), (0, pad_k)))
        keep = jnp.broadcast_to(valid.astype(jnp.int32)[:, None], (tokens, 8))

        returned = []
        for h in range(STAGES):
            done = expert_rows(counts_in, landed[h].reshape(slots, width), w_exp_gate, w_exp_up, w_exp_down, h * part, part, capacity)
            returned.append(lax.all_to_all(done.reshape(group, part, width), 'dpa', 0, 0, tiled=True))
        for h in range(STAGES):
            total = merge_rows(pos, gates, keep, total, returned[h].reshape(slots, width), h * slots, top_k, h == STAGES - 1)
        return total.reshape(x_in.shape), lat_upd.reshape(lat_cache.shape), rope_upd.reshape(rope_cache.shape)

    return jax.shard_map(device_step, mesh=mesh, in_specs=(tok_spec,) * 6 + (whole,) * 13 + (exp_spec,) * 3, out_specs=(tok_spec, tok_spec, tok_spec), check_vma=False)
```

```python
import functools

import jax
import jax.numpy as jnp
from jax import lax
from jax.experimental import pallas as pl
from jax.experimental.pallas import tpu as pltpu
from jax.sharding import PartitionSpec as P

EPS = 1e-6
THETA = 10000.0
UNIT = 16
STAGES = 2
LANES = 128
TILE = 256
HEADS_STEP = 2
PACK_TILE = 768
MERGE_TILE = 768
BIG = 60000000


def rms_norm(vals, gain):
    vals_f32 = vals.astype(jnp.float32)
    inv_rms = lax.rsqrt(jnp.mean(vals_f32 * vals_f32, axis=-1, keepdims=True) + EPS)
    return (vals_f32 * inv_rms * gain.astype(jnp.float32)).astype(jnp.bfloat16)


def nn_dot(lhs, rhs):
    return jnp.dot(lhs, rhs, preferred_element_type=jnp.float32)


def params(vmem=BIG):
    return pltpu.CompilerParams(vmem_limit_bytes=vmem)


def attn_kernel(ctx_ref, q_ref, uk_ref, uv_ref, lat_ref, kr_ref, cos_ref, sin_ref, out_ref, lat_t_ref, *, scale, nope):
    @pl.when(pl.program_id(0) == 0)
    def _():
        lat_t_ref[...] = lat_ref[...].T

    chunk = q_ref.shape[2]
    keys = lat_ref.shape[0]
    half = cos_ref.shape[0]
    block = min(TILE, chunk)
    chains = [(g, r) for g in range(q_ref.shape[0]) for r in range(chunk // block)]

    def seen(r):
        return keys - chunk + (r + 1) * block

    def scores_of(g, r):
        cols = slice(r * block, (r + 1) * block)
        q_lat = nn_dot(uk_ref[:, g * nope:(g + 1) * nope], q_ref[g, :nope, cols]).astype(jnp.bfloat16)
        first = q_ref[g, nope:nope + half, cols].astype(jnp.float32)
        second = q_ref[g, nope + half:, cols].astype(jnp.float32)
        cos_tab, sin_tab = cos_ref[:, cols], sin_ref[:, cols]
        q_rope = jnp.concatenate([first * cos_tab - second * sin_tab, second * cos_tab + first * sin_tab], axis=0).astype(jnp.bfloat16)
        return nn_dot(lat_ref[:seen(r), :], q_lat) + nn_dot(kr_ref[:seen(r), :], q_rope)

    def prob_of(scores, r):
        scores = scores * scale
        row_pos = lax.broadcasted_iota(jnp.int32, (1, block), 1) + (ctx_ref[0] + r * block)
        key_pos = lax.broadcasted_iota(jnp.int32, scores.shape, 0)
        scores = jnp.where(key_pos <= row_pos, scores, -1e30)
        expo = jnp.exp(scores - jnp.max(scores, axis=0, keepdims=True))
        return (expo * (1.0 / jnp.sum(expo, axis=0, keepdims=True))).astype(jnp.bfloat16)

    def finish(prob, g, r):
        vdim = out_ref.shape[1]
        out_lat = nn_dot(lat_t_ref[:, :seen(r)], prob).astype(jnp.bfloat16)
        out_ref[g, :, r * block:(r + 1) * block] = lax.dot_general(uv_ref[:, g * vdim:(g + 1) * vdim], out_lat, (((0,), (0,)), ((), ())), preferred_element_type=jnp.float32).astype(jnp.bfloat16)

    scores, probs = {0: scores_of(*chains[0])}, {}
    for i, (g, r) in enumerate(chains):
        if i + 1 < len(chains):
            scores[i + 1] = scores_of(*chains[i + 1])
        probs[i] = prob_of(scores.pop(i), r)
        if i > 0:
            finish(probs.pop(i - 1), *chains[i - 1])
    finish(probs.pop(len(chains) - 1), *chains[-1])


def attention(ctx, q_t, w_uk, w_uv, lat, kr, cos_t, sin_t, scale, nope):
    heads, qdim, chunk = q_t.shape
    keys, rank = lat.shape
    vdim = w_uv.shape[1] // heads
    rope = kr.shape[1]
    full = lambda arr: pl.BlockSpec(arr.shape, lambda h, c: (0, 0))
    head = lambda rows, cols: pl.BlockSpec((HEADS_STEP, rows, cols), lambda h, c: (h, 0, 0))
    spec = pltpu.PrefetchScalarGridSpec(
        num_scalar_prefetch=1, grid=(heads // HEADS_STEP,),
        in_specs=[head(qdim, chunk), pl.BlockSpec((rank, HEADS_STEP * nope), lambda h, c: (0, h)), pl.BlockSpec((rank, HEADS_STEP * vdim), lambda h, c: (0, h)),
                  full(lat), full(kr), full(cos_t), full(sin_t)],
        out_specs=head(vdim, chunk), scratch_shapes=[pltpu.VMEM((rank, keys), jnp.bfloat16)])
    flops = 2 * heads * chunk * (rank * (nope + vdim) + keys * (2 * rank + rope))
    return pl.pallas_call(
        functools.partial(attn_kernel, scale=scale, nope=nope), grid_spec=spec,
        out_shape=jax.ShapeDtypeStruct((heads, vdim, chunk), jnp.bfloat16), compiler_params=params(),
        cost_estimate=pl.CostEstimate(flops=flops, bytes_accessed=16 * 2**20, transcendentals=heads * chunk * keys),
        name='attend')(ctx, q_t, w_uk, w_uv, lat, kr, cos_t, sin_t)


def send_kernel(pos_ref, u_ref, out_ref, *, base, top_k):
    tile = out_ref.shape[0]
    tokens = u_ref.shape[0]
    slots = lax.broadcasted_iota(jnp.int32, (tile, tokens), 0) + (base + pl.program_id(0) * tile)
    hit = slots == pos_ref[0:1, :]
    for i in range(1, top_k):
        hit = hit | (slots == pos_ref[i:i + 1, :])
    pick = jnp.where(hit, 1.0, 0.0).astype(jnp.bfloat16)
    out_ref[...] = nn_dot(pick, u_ref[...]).astype(jnp.bfloat16)


def send_rows(pos_t, normed, slots, base, top_k):
    tokens, width = normed.shape
    tile = min(PACK_TILE, slots)
    return pl.pallas_call(
        functools.partial(send_kernel, base=base, top_k=top_k), grid=(slots // tile,),
        in_specs=[pl.BlockSpec(pos_t.shape, lambda k: (0, 0)), pl.BlockSpec((tokens, width), lambda k: (0, 0))],
        out_specs=pl.BlockSpec((tile, width), lambda k: (k, 0)),
        out_shape=jax.ShapeDtypeStruct((slots, width), jnp.bfloat16), compiler_params=params(),
        cost_estimate=pl.CostEstimate(flops=2 * slots * tokens * width, bytes_accessed=slots * width * 2, transcendentals=0),
        name='pack_rows')(pos_t, normed)


def expert_kernel(counts_ref, in_ref, gate_hbm, up_hbm, down_hbm, rows_ref, gate_v, up_v, down_v, x_v, y_v, ids, lows, highs, w_sem, in_sem, out_sem, *, first, part, capacity, sources):
    per_tile = x_v.shape[1] // UNIT
    per_source = part // UNIT
    total_units = sources * per_source
    stride = total_units + per_tile
    local_exp = 2

    def weights(e):
        return [pltpu.make_async_copy(src.at[e], dst.at[e], w_sem.at[e]) for src, dst in ((gate_hbm, gate_v), (up_hbm, up_v), (down_hbm, down_v))]

    for e in range(local_exp):
        for copy in weights(e):
            copy.start()

    def list_units(e):
        def step(source, count):
            filled = counts_ref[source, e]
            for j in range(per_source):
                start = first + j * UNIT
                low = 0 if e == 0 else capacity - filled - start
                high = filled - start if e == 0 else UNIT
                ids[e * stride + count] = source * per_source + j
                lows[e * stride + count] = low
                highs[e * stride + count] = high
                need = filled > start if e == 0 else capacity - filled < start + UNIT
                count = count + need.astype(jnp.int32)
            return count
        return lax.fori_loop(0, sources, step, jnp.int32(0))

    units0, units1 = list_units(0), list_units(1)
    tiles0 = lax.div(units0 + (per_tile - 1), per_tile)
    tiles = tiles0 + lax.div(units1 + (per_tile - 1), per_tile)

    def place(t):
        e = jnp.where(t >= tiles0, 1, 0)
        begin = (t - jnp.where(t >= tiles0, tiles0, 0)) * per_tile
        size = jnp.minimum(per_tile, jnp.where(t >= tiles0, units1, units0) - begin)
        return e, e * stride + begin, size

    def in_copy(t, i):
        where = ids[place(t)[1] + i]
        return pltpu.make_async_copy(rows_ref.at[pl.ds(pl.multiple_of(where * UNIT, UNIT), UNIT), :], x_v.at[t % 2, pl.ds(pl.multiple_of(i * UNIT, UNIT), UNIT), :], in_sem.at[t % 2])

    def out_copy(t, i):
        where = ids[place(t)[1] + i]
        return pltpu.make_async_copy(y_v.at[t % 2, pl.ds(pl.multiple_of(i * UNIT, UNIT), UNIT), :], rows_ref.at[pl.ds(pl.multiple_of(where * UNIT, UNIT), UNIT), :], out_sem.at[t % 2])

    def each(t, copy_of, wait):
        @pl.loop(0, place(t)[2])
        def _(i):
            copy = copy_of(t, i)
            copy.wait() if wait else copy.start()

    for copy in weights(0):
        copy.wait()

    @pl.loop(0, tiles)
    def _(t):
        switch = t == tiles0

        @pl.when(switch)
        def _():
            for copy in weights(1):
                copy.wait()

        @pl.when(switch & (t > 0))
        def _():
            each(t - 1, out_copy, True)

        @pl.when(switch | (t == 0))
        def _():
            each(t, in_copy, False)

        each(t, in_copy, True)

        @pl.when((t + 1 < tiles) & (t + 1 != tiles0))
        def _():
            each(t + 1, in_copy, False)

        e, begin, _ = place(t)
        slot = t % 2
        rows = x_v[slot]
        gate = nn_dot(rows, gate_v[e])
        up = nn_dot(rows, up_v[e])
        act = (jax.nn.silu(gate) * up).astype(jnp.bfloat16)
        res = nn_dot(act, down_v[e])
        for i in range(per_tile):
            span = slice(i * UNIT, (i + 1) * UNIT)
            line = lax.broadcasted_iota(jnp.int32, (UNIT, rows.shape[1]), 0)
            mine = (line >= lows[begin + i]) & (line < highs[begin + i])
            y_v[slot, span, :] = jnp.where(mine, res[span], rows[span].astype(jnp.float32)).astype(jnp.bfloat16)

        @pl.when((t > 0) & jnp.logical_not(switch))
        def _():
            each(t - 1, out_copy, True)

        each(t, out_copy, False)

    @pl.when(tiles == tiles0)
    def _():
        for copy in weights(1):
            copy.wait()

    @pl.when(tiles > 0)
    def _():
        each(tiles - 1, out_copy, True)


def expert_rows(counts, rows, w_gate, w_up, w_down, first, part, capacity):
    slots, width = rows.shape
    sources = counts.shape[0]
    local_exp, _, ff = w_gate.shape
    tile = min(TILE, slots)
    room = local_exp * (slots // UNIT + tile // UNIT)
    anywhere = pl.BlockSpec(memory_space=pl.ANY)
    return pl.pallas_call(
        functools.partial(expert_kernel, first=first, part=part, capacity=capacity, sources=sources),
        in_specs=[pl.BlockSpec(memory_space=pltpu.SMEM)] + [anywhere] * 4, out_specs=anywhere,
        out_shape=jax.ShapeDtypeStruct((slots, width), jnp.bfloat16), input_output_aliases={1: 0},
        scratch_shapes=[pltpu.VMEM(w_gate.shape, jnp.bfloat16), pltpu.VMEM(w_up.shape, jnp.bfloat16), pltpu.VMEM(w_down.shape, jnp.bfloat16),
                        pltpu.VMEM((2, tile, width), jnp.bfloat16), pltpu.VMEM((2, tile, width), jnp.bfloat16),
                        pltpu.SMEM((room,), jnp.int32), pltpu.SMEM((room,), jnp.int32), pltpu.SMEM((room,), jnp.int32),
                        pltpu.SemaphoreType.DMA((local_exp,)), pltpu.SemaphoreType.DMA((2,)), pltpu.SemaphoreType.DMA((2,))],
        compiler_params=params(),
        cost_estimate=pl.CostEstimate(flops=6 * slots * width * ff, bytes_accessed=12 * width * ff, transcendentals=0),
        name='expert_rows')(counts, rows, w_gate, w_up, w_down)


def merge_kernel(pos_ref, gate_ref, keep_ref, start_ref, rows_ref, out_ref, acc_ref, mix_ref, *, base, top_k, last):
    k = pl.program_id(0)

    @pl.when(k == 0)
    def _():
        acc_ref[...] = start_ref[...]

    tile = rows_ref.shape[0]
    tokens = acc_ref.shape[0]
    strip = 32
    for t in range(0, tokens, strip):
        at = slice(t, t + strip)
        spots = [jnp.broadcast_to(pos_ref[at, i:i + 1], (strip, LANES)) for i in range(top_k)]
        gates = [jnp.broadcast_to(gate_ref[at, i:i + 1], (strip, LANES)) for i in range(top_k)]
        for c in range(0, tile, LANES):
            slots = lax.broadcasted_iota(jnp.int32, (strip, LANES), 1) + (base + c + k * tile)
            mix = jnp.zeros((strip, LANES), jnp.float32)
            for i in range(top_k):
                mix = jnp.where(slots == spots[i], gates[i], mix)
            high = mix.astype(jnp.bfloat16)
            rest = mix - high.astype(jnp.float32)
            mid = rest.astype(jnp.bfloat16)
            low = (rest - mid.astype(jnp.float32)).astype(jnp.bfloat16)
            for n, piece in enumerate((high, mid, low)):
                mix_ref[n * tokens + t:n * tokens + t + strip, c:c + LANES] = piece
    width = acc_ref.shape[1]
    for j in range(0, width, TILE):
        parts = nn_dot(mix_ref[...], rows_ref[:, j:j + TILE])
        acc_ref[:, j:j + TILE] += parts[:tokens] + (parts[tokens:2 * tokens] + parts[2 * tokens:])

    @pl.when(k == pl.num_programs(0) - 1)
    def _():
        if last:
            out_ref[...] = jnp.where(keep_ref[:, 0:1] > 0, acc_ref[...], 0.0).astype(out_ref.dtype)
        else:
            out_ref[...] = acc_ref[...]


def merge_rows(pos, gates, keep, start, rows, base, top_k, last):
    slots, width = rows.shape
    tokens = start.shape[0]
    tile = min(MERGE_TILE, slots)
    full = lambda arr: pl.BlockSpec(arr.shape, lambda k: (0, 0))
    return pl.pallas_call(
        functools.partial(merge_kernel, base=base, top_k=top_k, last=last), grid=(slots // tile,),
        in_specs=[full(pos), full(gates), full(keep), full(start), pl.BlockSpec((tile, width), lambda k: (k, 0))],
        out_specs=pl.BlockSpec((tokens, width), lambda k: (0, 0)),
        out_shape=jax.ShapeDtypeStruct((tokens, width), jnp.bfloat16 if last else jnp.float32),
        scratch_shapes=[pltpu.VMEM((tokens, width), jnp.float32), pltpu.VMEM((3 * tokens, tile), jnp.bfloat16)], compiler_params=params(),
        cost_estimate=pl.CostEstimate(flops=6 * slots * tokens * width, bytes_accessed=slots * width * 2, transcendentals=0),
        name='merge_rows')(pos, gates, keep, start, rows)


def solution(mesh):
    group = mesh.shape['dpa']
    tok_spec = P(('dp', 'dpa'))
    whole = P()
    exp_spec = P('dpa')

    def device_step(x_in, chunk_len, ctx_len, lat_cache, rope_cache, topk_idx, g_attn, w_q, w_dkv, g_kv, w_kr, w_uk, w_uv, w_o, g_ffn, w_router, w_sh_gate, w_sh_up, w_sh_down, w_exp_gate, w_exp_up, w_exp_down):
        tokens, width = x_in.shape[2], x_in.shape[3]
        top_k = topk_idx.shape[-1]
        local_exp = w_exp_gate.shape[0]
        experts = group * local_exp
        capacity = tokens * top_k // group
        part = capacity // STAGES
        slots = group * part
        length = chunk_len[0, 0]
        ctx = ctx_len[0, 0]

        row_ids = jnp.arange(tokens, dtype=jnp.int32)
        valid = row_ids < length
        choice = topk_idx.reshape(tokens, top_k)
        picked = (choice[:, :, None] == jnp.arange(experts, dtype=jnp.int32)) & valid[:, None, None]
        member = jnp.any(picked, axis=1)
        before = (row_ids[:, None] > row_ids[None, :]).astype(jnp.bfloat16)
        rank_in = nn_dot(before, member.astype(jnp.bfloat16)).astype(jnp.int32)
        counts = jnp.sum(member.astype(jnp.int32), axis=0)
        counts_in = lax.all_to_all(counts.reshape(group, local_exp), 'dpa', 0, 0, tiled=True)
        ids = jnp.arange(experts, dtype=jnp.int32)
        place = jnp.where(ids % local_exp == 0, rank_in, capacity - 1 - rank_in)
        pos_all = (place // part) * slots + (ids // local_exp) * part + place % part
        pos = jnp.sum(jnp.where(picked, pos_all[:, None, :], 0), axis=2)
        pos = jnp.where(valid[:, None], pos, -1)
        pad_k = (-top_k) % 8
        pos = jnp.pad(pos, ((0, 0), (0, pad_k)), constant_values=-1)
        pos_t = pos.T

        chunk_x = x_in.reshape(tokens, width)
        normed_x = rms_norm(chunk_x, g_attn)
        rope_dim = w_kr.shape[1]
        heads, qdim = w_q.shape[1], w_q.shape[2]
        nope_dim = qdim - rope_dim
        half = rope_dim // 2
        q_t = jnp.einsum('cd,dhq->hqc', normed_x, w_q, preferred_element_type=jnp.float32).astype(jnp.bfloat16)
        inv_freq = THETA ** (-2.0 * jnp.arange(half, dtype=jnp.float32) / (2 * half))
        angle = (ctx + row_ids).astype(jnp.float32)[:, None] * inv_freq
        cos_tab, sin_tab = jnp.cos(angle), jnp.sin(angle)
        lat_new = rms_norm(nn_dot(normed_x, w_dkv), g_kv)
        kr_raw = nn_dot(normed_x, w_kr)
        kr_new = jnp.concatenate([kr_raw[:, :half] * cos_tab - kr_raw[:, half:] * sin_tab, kr_raw[:, half:] * cos_tab + kr_raw[:, :half] * sin_tab], axis=1).astype(jnp.bfloat16)

        def write_window(cache, new_rows):
            old_rows = lax.dynamic_slice_in_dim(cache, ctx, tokens, axis=0)
            return lax.dynamic_update_slice_in_dim(cache, jnp.where(valid[:, None], new_rows, old_rows), ctx, axis=0)

        lat_upd = write_window(lat_cache[0, 0], lat_new)
        rope_upd = write_window(rope_cache[0, 0], kr_new)
        out_head = attention(ctx_len.reshape(1), q_t, w_uk.reshape(w_uk.shape[0], -1), w_uv.reshape(w_uv.shape[0], -1), lat_upd, rope_upd, cos_tab.T, sin_tab.T, qdim ** -0.5, nope_dim)
        attn_out = jnp.einsum('hvc,hvd->cd', out_head, w_o, preferred_element_type=jnp.float32).astype(jnp.bfloat16)
        hidden = (chunk_x.astype(jnp.float32) + attn_out.astype(jnp.float32)).astype(jnp.bfloat16)
        normed = rms_norm(hidden, g_ffn)

        packed = [send_rows(pos_t, normed, slots, h * slots, top_k).reshape(group, part, width) for h in range(STAGES)]
        shared_act = (jax.nn.silu(nn_dot(normed, w_sh_gate)) * nn_dot(normed, w_sh_up)).astype(jnp.bfloat16)
        packed[1], shared_act = lax.optimization_barrier((packed[1], shared_act))
        landed = [lax.all_to_all(rows, 'dpa', 0, 0, tiled=True) for rows in packed]
        total = hidden.astype(jnp.float32) + nn_dot(shared_act, w_sh_down)
        route_prob = jax.nn.softmax(nn_dot(normed, w_router), axis=-1)
        gates = jnp.sum(jnp.where(picked, route_prob[:, None, :], 0.0), axis=2)
        gates = jnp.pad(gates, ((0, 0), (0, pad_k)))
        keep = jnp.broadcast_to(valid.astype(jnp.int32)[:, None], (tokens, 8))

        returned = []
        for h in range(STAGES):
            done = expert_rows(counts_in, landed[h].reshape(slots, width), w_exp_gate, w_exp_up, w_exp_down, h * part, part, capacity)
            returned.append(lax.all_to_all(done.reshape(group, part, width), 'dpa', 0, 0, tiled=True))
        for h in range(STAGES):
            total = merge_rows(pos, gates, keep, total, returned[h].reshape(slots, width), h * slots, top_k, h == STAGES - 1)
        return total.reshape(x_in.shape), lat_upd.reshape(lat_cache.shape), rope_upd.reshape(rope_cache.shape)

    return jax.shard_map(device_step, mesh=mesh, in_specs=(tok_spec,) * 6 + (whole,) * 13 + (exp_spec,) * 3, out_specs=(tok_spec, tok_spec, tok_spec), check_vma=False)
```
